32 devices in a mesh: parts: 2 (over y), replica: 4 (over x, core), tensor: 4 (over z).
Axes of the slice: x: 2, y: 2, z: 4, core: 2. Of those that a mesh axis runs over, the one named last changes fastest.
Arguments:
- prompt_owner: int32 [8], P('parts'), parts along dimension 0, may hold values from 0 to 3, each once
- fork_map: int32 [1024], P(('parts', 'replica')), parts along dimension 0, may hold values from 0 to 3
- page_table: int32 [24], P('parts'), parts along dimension 0, may hold values from 0 to 11, each once
- prompt_length: int32 [8], P('parts'), parts along dimension 0, may hold values from 1 to 384
- span_states: bfloat16 [1024, 8192], P(('parts', 'replica'), 'tensor'), parts along dimension 0, may hold values from -6 to 6
- decode_states: bfloat16 [1024, 4, 8192], P(('parts', 'replica'), None, 'tensor'), parts along dimension 0, may hold values from -6 to 6
- decode_queries: bfloat16 [1024, 4, 4096], P(('parts', 'replica'), None, 'tensor'), parts along dimension 0, may hold values from -64 to 64
- key_weight: bfloat16 [8192, 512], P('tensor'), may hold values from -0.0625 to 0.0625
- value_weight: bfloat16 [8192, 512], P('tensor'), may hold values from -0.0625 to 0.0625
- out_weight: bfloat16 [4096, 8192], P(None, 'tensor'), may hold values from -0.09375 to 0.09375
- page_pool: bfloat16 [4, 24, 128, 256], P('tensor', 'parts'), parts along dimension 1, may hold values from -6 to 60, as said below
Outputs:
- decoded: bfloat16 [1024, 4, 8192], P(('parts', 'replica'), None, 'tensor'), parts along dimension 0
The draws below stay inside these ranges and needn't reach their ends.
There are 2 independent parts, one for each index of `parts`. The reference program is written for one: setup_inputs(seed, part) draws one part's arguments, and reference() takes and returns one part's arrays. A program takes and returns all parts, laid end to end along the dimension named above; an argument that names none is the same for every part. Nothing has to cross between parts.
Inputs may be any that keep to these rules, and one draw needn't show every extreme that they name: Replica r prefills prompt prompt_owner[r]; every prompt has exactly one such replica. The cache pages of prompt p are page_table[p * 3 + c] for c below 3; every pool page belongs to exactly one prompt. page_pool[t] holds the cache of key-value head t; devices that read the same head hold equal copies.
All inputs are finite; a program needn't handle non-finite values.
Results may differ from the reference program's by a relative error of at most 0.009.
Values may be sent and summed in bfloat16 or wider, within the bound.
A program may use at most 64 MiB of HBM per device.

```python
import jax
import jax.numpy as jnp
from jax import lax

D = 8192
HD = 128
HEADS = 32
KVH = 4
SPAN = 128
STEPS = 4
PAGE = 128
CPAGES = 3
ROWS = 128
SHARE = 1
POOL = 12
ALL_ROWS = 512
ALL_SPAN = 512
N_REPLICA = 4


def draw_page_pool(key, part):
    base = jnp.clip(jax.random.normal(key, (KVH, POOL, PAGE, 2 * HD), jnp.float32), -6.0, 6.0)
    return jnp.repeat(base, SHARE, axis=0).astype(jnp.bfloat16)


def draw_decode_queries(key, part):
    base = jnp.clip(jax.random.normal(key, (ALL_ROWS, STEPS, HEADS, HD), jnp.float32), -6.0, 6.0)
    return base.reshape(ALL_ROWS, STEPS, HEADS * HD).astype(jnp.bfloat16)


def set_ends(drawn, key, smallest, high):
    index_at = [jax.random.randint(jax.random.fold_in(key, axis), (), 0, length) for axis, length in enumerate(drawn.shape)]
    main_axis = drawn.shape.index(max(drawn.shape))
    next_to = index_at[:main_axis] + [(index_at[main_axis] + 1) % drawn.shape[main_axis]] + index_at[main_axis + 1:]
    return drawn.at[tuple(index_at)].set(smallest).at[tuple(next_to)].set(high)


def steps_of(rng, extent, cuts, low, top_value):
    def one(axis_at, shards_of):
        heights = jax.random.uniform(jax.random.fold_in(jax.random.fold_in(rng, 6), axis_at), (shards_of,), jnp.float32, low / len(cuts), top_value / len(cuts))
        return jnp.repeat(jnp.exp(heights), extent[axis_at] // shards_of).reshape((-1,) + (1,) * (len(extent) - axis_at - 1))

    loudness = one(*cuts[0])
    for cut in cuts[1:]:
        loudness = loudness * one(*cut)
    return loudness


def normal_values(key, shape, spread, bound, cuts=(), kind=jnp.bfloat16):
    values = spread * jax.random.normal(key, shape, jnp.float32)
    if cuts:
        values = values * steps_of(key, shape, cuts, -0.22, 0.18)
    return jnp.clip(values, -bound, bound).astype(kind)


def setup_inputs(seed: int = 0, part: int = 0) -> dict:
    key_list = jax.random.split(jax.random.key(seed), 12)
    part_splits = jax.random.split(jax.random.fold_in(key_list[11], part), 12)
    prompt_owner = jax.random.permutation(part_splits[0], N_REPLICA).astype(jnp.int32)
    fork_map = set_ends(jax.random.randint(part_splits[1], (ALL_ROWS,), 0, N_REPLICA), jax.random.fold_in(part_splits[1], 1), 0, N_REPLICA - 1).astype(jnp.int32)
    page_table = jax.random.permutation(part_splits[2], POOL).astype(jnp.int32)
    prompt_length = set_ends(jax.random.randint(part_splits[3], (N_REPLICA,), 1, CPAGES * PAGE + 1), jax.random.fold_in(part_splits[3], 1), 1, CPAGES * PAGE).astype(jnp.int32)
    span_states = normal_values(part_splits[4], (ALL_SPAN, D), 1.0, 6.0, ((0, 4), (1, 4)))
    decode_states = normal_values(part_splits[5], (ALL_ROWS, STEPS, D), 1.0, 6.0, ((0, 4), (2, 4)))
    decode_queries = draw_decode_queries(jax.random.fold_in(jax.random.fold_in(key_list[11], part), 71), part)
    key_weight = normal_values(key_list[7], (D, KVH * HD), D ** -0.5, 0.0625, ((0, 4),))
    value_weight = normal_values(key_list[8], (D, KVH * HD), D ** -0.5, 0.0625, ((0, 4),))
    out_weight = normal_values(key_list[9], (HEADS * HD, D), (HEADS * HD) ** -0.5, 0.09375, ((1, 4),))
    page_pool = draw_page_pool(jax.random.fold_in(jax.random.fold_in(key_list[11], part), 71), part)
    return dict(prompt_owner=prompt_owner, fork_map=fork_map, page_table=page_table, prompt_length=prompt_length, span_states=span_states, decode_states=decode_states, decode_queries=decode_queries, key_weight=key_weight, value_weight=value_weight, out_weight=out_weight, page_pool=page_pool)


rope_base = 1000000.0


def rotary(vectors, places):
    half = vectors.shape[-1] // 2
    freq = rope_base ** (-(2.0 / vectors.shape[-1]) * jnp.arange(half, dtype=jnp.float32))
    angle = places.astype(jnp.float32)[..., None, None] * freq
    cosine = jnp.cos(angle)
    sine = jnp.sin(angle)
    first = vectors[..., :half]
    second = vectors[..., half:]
    return jnp.concatenate([first * cosine - second * sine, second * cosine + first * sine], -1)


def reference(prompt_owner, fork_map, page_table, prompt_length, span_states, decode_states, decode_queries, key_weight, value_weight, out_weight, page_pool):
    weights = jnp.concatenate([key_weight, value_weight], 1)
    tokens = jnp.concatenate([span_states, decode_states.reshape(ALL_ROWS * STEPS, D)], 0)
    projected = jnp.dot(tokens, weights, preferred_element_type=jnp.float32)
    span_places = prompt_length[prompt_owner][:, None] + jnp.arange(SPAN, dtype=jnp.int32)[None, :]
    tail_places = prompt_length[fork_map][:, None] + SPAN + jnp.arange(STEPS, dtype=jnp.int32)[None, :]
    positions = jnp.concatenate([span_places.reshape(-1), tail_places.reshape(-1)]).astype(jnp.int32)
    number = positions.shape[0]
    new_keys = rotary(projected[:, :KVH * HD].reshape(number, KVH, HD), positions).astype(jnp.bfloat16)
    new_values = projected[:, KVH * HD:].reshape(number, KVH, HD).astype(jnp.bfloat16)
    span_keys = new_keys[:ALL_SPAN]
    span_values = new_values[:ALL_SPAN]
    tail_keys = new_keys[ALL_SPAN:].reshape(N_REPLICA, ROWS, STEPS, KVH, HD)
    tail_values = new_values[ALL_SPAN:].reshape(N_REPLICA, ROWS, STEPS, KVH, HD)
    entries = jnp.arange(POOL, dtype=jnp.int32)
    page_prompt = jnp.zeros((POOL,), jnp.int32).at[page_table].set(entries // CPAGES)
    page_slot = jnp.zeros((POOL,), jnp.int32).at[page_table].set(entries % CPAGES)
    cached_places = page_slot[:, None] * PAGE + jnp.arange(PAGE, dtype=jnp.int32)[None, :]
    visible = cached_places < prompt_length[page_prompt][:, None]
    pool_prompt = jnp.where(visible, page_prompt[:, None], -1).reshape(-1)
    key_prompt = jnp.concatenate([pool_prompt, jnp.repeat(prompt_owner, SPAN)]).astype(jnp.int32)
    group = HEADS // KVH
    scale = HD ** -0.5
    causal = jnp.arange(STEPS)[None, :] <= jnp.arange(STEPS)[:, None]
    queries = decode_queries.reshape(N_REPLICA, ROWS, STEPS, HEADS, HD)
    row_prompts = fork_map.reshape(N_REPLICA, ROWS)

    def one_replica(items):
        query, prompt, own_keys, own_values = items
        pieces = []
        for head_group in range(KVH):
            cache = page_pool[head_group * SHARE].reshape(POOL * PAGE, 2 * HD)
            key_table = jnp.concatenate([cache[:, :HD], span_keys[:, head_group]], 0).astype(jnp.float32)
            value_table = jnp.concatenate([cache[:, HD:], span_values[:, head_group]], 0).astype(jnp.float32)
            local = query[:, :, head_group * group:(head_group + 1) * group].astype(jnp.float32)
            scores = jnp.einsum("rshd,kd->rshk", local, key_table) * scale
            allowed = (key_prompt[None, :] == prompt[:, None])[:, None, None, :]
            scores = jnp.where(allowed, scores, -jnp.inf)
            tail_key = own_keys[:, :, head_group].astype(jnp.float32)
            tail_value = own_values[:, :, head_group].astype(jnp.float32)
            tail = jnp.einsum("rshd,rtd->rsht", local, tail_key) * scale
            tail = jnp.where(causal[None, :, None, :], tail, -jnp.inf)
            highest = jnp.maximum(jnp.max(scores, -1), jnp.max(tail, -1))
            weight = jnp.exp(scores - highest[..., None])
            tail_weight = jnp.exp(tail - highest[..., None])
            total = jnp.sum(weight, -1) + jnp.sum(tail_weight, -1)
            mixed = jnp.einsum("rshk,kd->rshd", weight.astype(jnp.bfloat16).astype(jnp.float32), value_table)
            mixed = mixed + jnp.einsum("rsht,rtd->rshd", tail_weight.astype(jnp.bfloat16).astype(jnp.float32), tail_value)
            pieces.append((mixed / total[..., None]).astype(jnp.bfloat16))
        return jnp.concatenate(pieces, 2)

    attended = lax.map(one_replica, (queries, row_prompts, tail_keys, tail_values))
    flat = attended.reshape(ALL_ROWS * STEPS, HEADS * HD)
    decoded = jnp.dot(flat, out_weight, preferred_element_type=jnp.float32).astype(jnp.bfloat16)
    return decoded.reshape(ALL_ROWS, STEPS, D)
```

```python
import functools
import math

import jax
import jax.numpy as jnp
from jax import lax
from jax.experimental import pallas as pl
from jax.experimental.pallas import tpu as pltpu
from jax.sharding import PartitionSpec as P

HD = 128


rope_base = 1000000.0


def rotary(vectors, places):
    half = vectors.shape[-1] // 2
    freq = rope_base ** (-(2.0 / vectors.shape[-1]) * jnp.arange(half, dtype=jnp.float32))
    angle = places.astype(jnp.float32)[..., None, None] * freq
    cosine = jnp.cos(angle)
    sine = jnp.sin(angle)
    first = vectors[..., :half]
    second = vectors[..., half:]
    return jnp.concatenate([first * cosine - second * sine, second * cosine + first * sine], -1)


def rotate_round(summed, places, kv_heads):
    number = summed.shape[0]
    turned = rotary(summed[:, : kv_heads * HD].reshape(number, kv_heads, HD), places)
    turned = turned.astype(jnp.bfloat16).reshape(number, kv_heads * HD)
    return jnp.concatenate([turned, summed[:, kv_heads * HD :].astype(jnp.bfloat16)], 1)


def own_pair(packed, head_group, kv_heads):
    key_part = lax.dynamic_slice_in_dim(packed, head_group * HD, HD, 1)
    value_part = lax.dynamic_slice_in_dim(packed, (kv_heads + head_group) * HD, HD, 1)
    return jnp.concatenate([key_part, value_part], 1)


def general(
    prompt_owner,
    fork_map,
    page_table,
    prompt_length,
    span_states,
    decode_states,
    decode_queries,
    key_weight,
    value_weight,
    out_weight,
    page_pool,
):
    replica = lax.axis_index("replica")
    device_rank = lax.axis_index("tensor")
    n_replica = lax.axis_size("replica")
    n_tensor = lax.axis_size("tensor")
    span = span_states.shape[0]
    rows, steps, width = decode_states.shape
    heads_dev = decode_queries.shape[2] // HD
    kv_heads = key_weight.shape[1] // HD
    sharing = n_tensor // kv_heads
    prompts = jnp.arange(n_replica, dtype=jnp.int32)
    own_prompt = jnp.sum(jnp.where(prompts == replica, prompt_owner, 0))
    own_length = jnp.sum(jnp.where(prompts == own_prompt, prompt_length, 0))
    row_hits = fork_map[:, None] == prompts[None, :]
    row_length = jnp.sum(jnp.where(row_hits, prompt_length[None, :], 0), 1)
    positions = jnp.concatenate(
        [
            own_length + jnp.arange(span, dtype=jnp.int32),
            (row_length[:, None] + span + jnp.arange(steps, dtype=jnp.int32)[None, :]).reshape(-1),
        ]
    )
    tokens = jnp.concatenate([span_states, decode_states.reshape(rows * steps, width)], 0)
    projected = jnp.dot(
        tokens, jnp.concatenate([key_weight, value_weight], 1), preferred_element_type=jnp.float32
    )
    share = lax.psum_scatter(projected, "tensor", scatter_dimension=0, tiled=True)
    number = share.shape[0]
    start = device_rank * number
    places = lax.dynamic_slice_in_dim(positions, start, number)
    turned = rotate_round(share, places, kv_heads)
    groups = jnp.stack(
        [own_pair(turned, group_index, kv_heads) for group_index in range(kv_heads)], 0
    )
    outgoing = jnp.repeat(groups, sharing, axis=0)
    paired = lax.all_to_all(outgoing, "tensor", split_axis=0, concat_axis=1, tiled=True).reshape(
        -1, 2 * HD
    )
    arrived = lax.all_gather(paired[:span], "replica", axis=0, tiled=True)
    tail_pair = paired[span:].reshape(rows, steps, 2 * HD)
    pool_pages = page_table.shape[0]
    cpages = pool_pages // n_replica
    page_size = page_pool.shape[2]
    entries = jnp.arange(pool_pages, dtype=jnp.int32)
    page_hits = page_table[None, :] == entries[:, None]
    page_prompt = jnp.sum(jnp.where(page_hits, entries[None, :] // cpages, 0), 1)
    page_slot = jnp.sum(jnp.where(page_hits, entries[None, :] % cpages, 0), 1)
    page_length = jnp.sum(
        jnp.where(page_prompt[:, None] == prompts[None, :], prompt_length[None, :], 0), 1
    )
    visible = (
        page_slot[:, None] * page_size + jnp.arange(page_size, dtype=jnp.int32)[None, :]
        < page_length[:, None]
    )
    pool_prompt = jnp.where(visible, page_prompt[:, None], -1).reshape(-1)
    key_prompt = jnp.concatenate([pool_prompt, jnp.repeat(prompt_owner, span)])
    key_table = jnp.concatenate([page_pool.reshape(-1, 2 * HD), arrived], 0)
    cached_keys = key_table[:, :HD]
    cached_values = key_table[:, HD:]
    scale = 1.0 / math.sqrt(HD)
    causal = jnp.arange(steps)[None, :] <= jnp.arange(steps)[:, None]
    per_block = max(1, min(rows, 512 // (steps * heads_dev)))
    blocks = rows // per_block
    queries = decode_queries.reshape(blocks, per_block, steps, heads_dev, HD)

    def attend(items):
        query, prompt, own_tail = items
        flat = query.reshape(-1, HD)
        scores = (
            lax.dot_general(
                flat, cached_keys, (((1,), (1,)), ((), ())), preferred_element_type=jnp.float32
            )
            * scale
        )
        scores = scores.reshape(per_block, steps, heads_dev, -1)
        allowed = (key_prompt[None, :] == prompt[:, None])[:, None, None, :]
        scores = jnp.where(allowed, scores, -jnp.inf)
        tail_scores = (
            jnp.einsum(
                "rshd,rtd->rsht", query, own_tail[..., :HD], preferred_element_type=jnp.float32
            )
            * scale
        )
        tail_scores = jnp.where(causal[None, :, None, :], tail_scores, -jnp.inf)
        highest = jnp.maximum(jnp.max(scores, -1), jnp.max(tail_scores, -1))
        weight = jnp.exp(scores - highest[..., None])
        tail_weight = jnp.exp(tail_scores - highest[..., None])
        total = jnp.sum(weight, -1) + jnp.sum(tail_weight, -1)
        rounded = weight.astype(jnp.bfloat16).reshape(-1, weight.shape[-1])
        mixed = jnp.dot(rounded, cached_values, preferred_element_type=jnp.float32).reshape(
            per_block, steps, heads_dev, HD
        )
        mixed = mixed + jnp.einsum(
            "rsht,rtd->rshd",
            tail_weight.astype(jnp.bfloat16),
            own_tail[..., HD:],
            preferred_element_type=jnp.float32,
        )
        return (mixed / total[..., None]).astype(jnp.bfloat16)

    attended = lax.map(
        attend,
        (
            queries,
            fork_map.reshape(blocks, per_block),
            tail_pair.reshape(blocks, per_block, steps, 2 * HD),
        ),
    )
    head_rows = attended.reshape(rows * steps, heads_dev * HD)
    decoded = jnp.dot(
        lax.all_gather(head_rows, "tensor", axis=1, tiled=True),
        out_weight,
        preferred_element_type=jnp.float32,
    )
    return decoded.astype(jnp.bfloat16).reshape(rows, steps, width)


MESH_ID = pl.DeviceIdType.MESH
TILE = 128
FAR = -(2.0**100)


def nt(left, right):
    return lax.dot_general(
        left, right, (((1,), (1,)), ((), ())), preferred_element_type=jnp.float32
    )


def fused(
    n, n_rep, steps, tok, wk, wv, cosine, sine, query, hot, pool, far, w_hbm, out,
    w_all, part, landed, own, span_all, keys, values, tail_key, tail_value, gathered, acc,
    w_sem, rs_send, rs_recv, sp_send, sp_recv, ag_send, ag_recv,
):
    z = lax.axis_index("tensor")
    rep = lax.axis_index("replica")
    span = span_all.shape[1]
    rows = query.shape[0]
    width = query.shape[1]
    heads = width // HD
    cached = pool.shape[0]
    blocks = tok.shape[0] // TILE
    span_blocks = span // TILE
    chunks = rows // TILE

    w_copy = pltpu.make_async_copy(w_hbm, w_all, w_sem)
    w_copy.start()
    barrier = pltpu.get_barrier_semaphore()
    for k in range(1, n):
        pl.semaphore_signal(
            barrier, inc=1, device_id={"tensor": lax.rem(z + k, n)}, device_id_type=MESH_ID
        )
    for k in range(1, n_rep):
        pl.semaphore_signal(
            barrier, inc=1, device_id={"replica": lax.rem(rep + k, n_rep)}, device_id_type=MESH_ID
        )
    pl.semaphore_wait(barrier, n + n_rep - 2)

    def at(block):
        return pl.ds(pl.multiple_of(block * TILE, TILE), TILE)

    def rs_copy(k, block):
        return pltpu.make_async_remote_copy(
            src_ref=part.at[k - 1, at(block)],
            dst_ref=landed.at[k - 1, at(block)],
            send_sem=rs_send.at[k - 1, block],
            recv_sem=rs_recv.at[k - 1, block],
            device_id={"tensor": lax.rem(z + k, n)},
            device_id_type=MESH_ID,
        )

    def project(block, owner):
        column = pl.ds(pl.multiple_of(owner * HD, HD), HD)
        weight = jnp.concatenate([wk[:, column], wv[:, column]], 1)
        return jnp.dot(tok[at(block), :], weight, preferred_element_type=jnp.float32)

    @pl.loop(0, blocks)
    def _(block):
        for k in range(1, n):
            part[k - 1, at(block), :] = project(block, lax.rem(z + k, n)).astype(jnp.bfloat16)
            rs_copy(k, block).start()

    @pl.loop(0, blocks)
    def _(block):
        own[at(block), :] = project(block, z)

    keys[:cached, :HD] = pool[:, :HD]
    values[:cached, :HD] = pool[:, HD:]
    keys[:, HD:] = far[...]
    values[:, HD:] = jnp.ones((values.shape[0], HD), jnp.bfloat16)
    tail_value[:, HD:] = jnp.ones((TILE, HD), jnp.bfloat16)

    def reduced(block):
        total = own[at(block), :]
        for k in range(1, n):
            rs_copy(k, block).wait_recv()
            total = total + landed[k - 1, at(block), :].astype(jnp.float32)
        key = total[:, :HD]
        key = key * cosine[at(block), :] + pltpu.roll(key, HD // 2, 1) * sine[at(block), :]
        return key.astype(jnp.bfloat16), total[:, HD:].astype(jnp.bfloat16)

    @pl.loop(0, span_blocks)
    def _(block):
        key, value = reduced(block)
        span_all[rep, at(block), :HD] = key
        span_all[rep, at(block), HD:] = value

    def sp_copy(k, whose):
        return pltpu.make_async_remote_copy(
            src_ref=span_all.at[whose],
            dst_ref=span_all.at[whose],
            send_sem=sp_send.at[k - 1],
            recv_sem=sp_recv.at[k - 1],
            device_id={"replica": lax.rem(rep + k, n_rep)},
            device_id_type=MESH_ID,
        )

    for k in range(1, n_rep):
        sp_copy(k, rep).start()
    for k in range(1, n_rep):
        sp_copy(k, lax.rem(rep - k + n_rep, n_rep)).wait_recv()
    for p in range(n_rep):
        keys[cached + p * span : cached + (p + 1) * span, :HD] = span_all[p, :, :HD]
        values[cached + p * span : cached + (p + 1) * span, :HD] = span_all[p, :, HD:]

    def ag_copy(side, distance, chunk, origin):
        target = z + 1 if side == 0 else z - 1
        return pltpu.make_async_remote_copy(
            src_ref=gathered.at[origin, at(chunk)],
            dst_ref=gathered.at[origin, at(chunk)],
            send_sem=ag_send.at[side, distance - 1, chunk],
            recv_sem=ag_recv.at[side, distance - 1, chunk],
            device_id={"tensor": target},
            device_id_type=MESH_ID,
        )

    line = lax.broadcasted_iota(jnp.int32, (TILE, TILE), 0)
    lane = lax.broadcasted_iota(jnp.int32, (TILE, TILE), 1)
    causal = (line // steps == lane // steps) & (lane <= line)
    factor = math.log2(math.e) / math.sqrt(HD)

    @pl.loop(0, chunks)
    def _(chunk):
        key, value = reduced(chunk + span_blocks)
        tail_key[...] = key
        tail_value[:, :HD] = value

        @pl.loop(0, heads)
        def _(head):
            column = pl.ds(pl.multiple_of(head * HD, HD), HD)
            asked = query[at(chunk), column]
            scores = nt(jnp.concatenate([asked, hot[at(chunk), :]], 1), keys[...])
            tail = jnp.where(causal, nt(asked, tail_key[...]), FAR)
            highest = jnp.maximum(
                jnp.max(scores, 1, keepdims=True), jnp.max(tail, 1, keepdims=True)
            )
            weight = jnp.exp2((scores - highest) * factor).astype(jnp.bfloat16)
            tail_weight = jnp.exp2((tail - highest) * factor).astype(jnp.bfloat16)
            mixed = jnp.dot(weight, values[...], preferred_element_type=jnp.float32) + jnp.dot(
                tail_weight, tail_value[...], preferred_element_type=jnp.float32
            )
            gathered[z, at(chunk), column] = (mixed[:, :HD] / mixed[:, HD:]).astype(jnp.bfloat16)

        @pl.when(z + 1 < n)
        def _():
            ag_copy(0, 1, chunk, z).start()

        @pl.when(z > 0)
        def _():
            ag_copy(1, 1, chunk, z).start()

    w_copy.wait()
    tall = min(2 * TILE, rows)
    per = tall // TILE
    wide = min(512, out.shape[1])

    def add(origin, half, first):
        span_rows = pl.ds(pl.multiple_of(half * tall, tall), tall)
        deep = pl.ds(pl.multiple_of(origin * width, width), width)

        @pl.loop(0, out.shape[1] // wide)
        def _(column):
            cols = pl.ds(pl.multiple_of(column * wide, wide), wide)
            term = jnp.dot(
                gathered[origin, span_rows, :], w_all[deep, cols], preferred_element_type=jnp.float32
            )
            if first:
                acc[span_rows, cols] = term
            else:
                acc[span_rows, cols] += term

    @pl.loop(0, rows // tall)
    def _(half):
        add(z, half, True)

    for distance in range(1, n):

        @pl.loop(0, rows // tall)
        def _(half):
            for side, origin, inside, onward in (
                (0, z - distance, z >= distance, z + 1 < n),
                (1, z + distance, z + distance < n, z > 0),
            ):
                for piece in range(per):
                    chunk = half * per + piece

                    @pl.when(inside)
                    def _():
                        ag_copy(side, distance, chunk, origin).wait_recv()

                    if distance < n - 1:

                        @pl.when(inside & onward)
                        def _():
                            ag_copy(side, distance + 1, chunk, origin).start()

            for side, origin, inside in (
                (0, z - distance, z >= distance),
                (1, z + distance, z + distance < n),
            ):

                @pl.when(inside)
                def _():
                    add(origin, half, False)

    @pl.loop(0, chunks)
    def _(chunk):
        out[at(chunk), :] = acc[at(chunk), :].astype(jnp.bfloat16)

    for k in range(1, n):

        @pl.loop(0, blocks)
        def _(block):
            rs_copy(k, block).wait_send()

    for k in range(1, n_rep):
        sp_copy(k, rep).wait_send()
    for distance in range(1, n):

        @pl.loop(0, chunks)
        def _(chunk):
            @pl.when((z >= distance - 1) & (z + 1 < n))
            def _():
                ag_copy(0, distance, chunk, z - distance + 1).wait_send()

            @pl.when((z + distance - 1 < n) & (z > 0))
            def _():
                ag_copy(1, distance, chunk, z + distance - 1).wait_send()


def on_device(
    prompt_owner,
    fork_map,
    page_table,
    prompt_length,
    span_states,
    decode_states,
    decode_queries,
    key_weight,
    value_weight,
    out_weight,
    page_pool,
):
    replica = lax.axis_index("replica")
    n_replica = lax.axis_size("replica")
    n_tensor = lax.axis_size("tensor")
    span = span_states.shape[0]
    rows, steps, width = decode_states.shape
    heads_dev = decode_queries.shape[2] // HD
    kv_heads = key_weight.shape[1] // HD
    number = rows * steps
    if (
        kv_heads != n_tensor
        or span % TILE
        or number % TILE
        or number % min(2 * TILE, number)
        or TILE % steps
        or n_replica > HD
    ):
        return general(
            prompt_owner, fork_map, page_table, prompt_length, span_states, decode_states,
            decode_queries, key_weight, value_weight, out_weight, page_pool,
        )
    prompts = jnp.arange(n_replica, dtype=jnp.int32)
    own_prompt = jnp.sum(jnp.where(prompts == replica, prompt_owner, 0))
    own_length = jnp.sum(jnp.where(prompts == own_prompt, prompt_length, 0))
    row_hits = fork_map[:, None] == prompts[None, :]
    row_length = jnp.sum(jnp.where(row_hits, prompt_length[None, :], 0), 1)
    positions = jnp.concatenate(
        [
            own_length + jnp.arange(span, dtype=jnp.int32),
            (row_length[:, None] + span + jnp.arange(steps, dtype=jnp.int32)[None, :]).reshape(-1),
        ]
    )
    half = HD // 2
    freq = rope_base ** (-(2.0 / HD) * jnp.arange(half, dtype=jnp.float32))
    angle = positions.astype(jnp.float32)[:, None] * freq
    cosine = jnp.cos(angle)
    sine = jnp.sin(angle)
    cosine = jnp.concatenate([cosine, cosine], 1)
    sine = jnp.concatenate([-sine, sine], 1)
    tokens = jnp.concatenate([span_states, decode_states.reshape(number, width)], 0)
    pool_pages = page_table.shape[0]
    cpages = pool_pages // n_replica
    page_size = page_pool.shape[2]
    entries = jnp.arange(pool_pages, dtype=jnp.int32)
    page_hits = page_table[None, :] == entries[:, None]
    page_prompt = jnp.sum(jnp.where(page_hits, entries[None, :] // cpages, 0), 1)
    page_slot = jnp.sum(jnp.where(page_hits, entries[None, :] % cpages, 0), 1)
    page_length = jnp.sum(
        jnp.where(page_prompt[:, None] == prompts[None, :], prompt_length[None, :], 0), 1
    )
    visible = (
        page_slot[:, None] * page_size + jnp.arange(page_size, dtype=jnp.int32)[None, :]
        < page_length[:, None]
    )
    pool_prompt = jnp.where(visible, page_prompt[:, None], -1).reshape(-1)
    key_prompt = jnp.concatenate([pool_prompt, jnp.repeat(prompt_owner, span)])
    lanes = jnp.arange(HD, dtype=jnp.int32)
    far = jnp.where(
        (lanes[None, :] < n_replica) & (key_prompt[:, None] != lanes[None, :]), FAR, 0.0
    ).astype(jnp.bfloat16)
    hot = jnp.broadcast_to(
        (fork_map[:, None] == lanes[None, :])[:, None, :], (rows, steps, HD)
    ).reshape(number, HD).astype(jnp.bfloat16)
    pool = page_pool.reshape(-1, 2 * HD)
    query = decode_queries.reshape(number, heads_dev * HD)
    features = out_weight.shape[1]
    table = pool.shape[0] + n_replica * span
    total = span + number
    vmem = pl.BlockSpec(memory_space=pltpu.VMEM)
    bf16, f32 = jnp.bfloat16, jnp.float32
    decoded = pl.pallas_call(
        functools.partial(fused, n_tensor, n_replica, steps),
        name="fused",
        out_shape=jax.ShapeDtypeStruct((number, features), bf16),
        in_specs=[vmem] * 9 + [pl.BlockSpec(memory_space=pl.ANY)],
        out_specs=vmem,
        scratch_shapes=[
            pltpu.VMEM(out_weight.shape, bf16),
            pltpu.VMEM((n_tensor - 1, total, 2 * HD), bf16),
            pltpu.VMEM((n_tensor - 1, total, 2 * HD), bf16),
            pltpu.VMEM((total, 2 * HD), f32),
            pltpu.VMEM((n_replica, span, 2 * HD), bf16),
            pltpu.VMEM((table, 2 * HD), bf16),
            pltpu.VMEM((table, 2 * HD), bf16),
            pltpu.VMEM((TILE, HD), bf16),
            pltpu.VMEM((TILE, 2 * HD), bf16),
            pltpu.VMEM((n_tensor, number, heads_dev * HD), bf16),
            pltpu.VMEM((number, features), f32),
            pltpu.SemaphoreType.DMA,
            pltpu.SemaphoreType.DMA((n_tensor - 1, total // TILE)),
            pltpu.SemaphoreType.DMA((n_tensor - 1, total // TILE)),
            pltpu.SemaphoreType.DMA((n_replica - 1,)),
            pltpu.SemaphoreType.DMA((n_replica - 1,)),
            pltpu.SemaphoreType.DMA((2, n_tensor - 1, number // TILE)),
            pltpu.SemaphoreType.DMA((2, n_tensor - 1, number // TILE)),
        ],
        compiler_params=pltpu.CompilerParams(
            collective_id=0, has_side_effects=True, vmem_limit_bytes=60 * 1024 * 1024
        ),
    )(tokens, key_weight, value_weight, cosine, sine, query, hot, pool, far, out_weight)
    return decoded.reshape(rows, steps, features)


def solution(mesh):
    in_specs = (
        P("parts"),
        P(("parts", "replica")),
        P("parts"),
        P("parts"),
        P(("parts", "replica"), "tensor"),
        P(("parts", "replica"), None, "tensor"),
        P(("parts", "replica"), None, "tensor"),
        P("tensor", None),
        P("tensor", None),
        P(None, "tensor"),
        P("tensor", "parts", None, None),
    )
    out_specs = P(("parts", "replica"), None, "tensor")
    return jax.shard_map(
        on_device, mesh=mesh, in_specs=in_specs, out_specs=out_specs, check_vma=False
    )
```

```python
import functools
import math

import jax
import jax.numpy as jnp
import numpy as np
from jax import lax
from jax.experimental import pallas as pl
from jax.experimental.pallas import tpu as pltpu
from jax.sharding import PartitionSpec as P

HD = 128


rope_base = 1000000.0


def rotary(vectors, places):
    half = vectors.shape[-1] // 2
    freq = rope_base ** (-(2.0 / vectors.shape[-1]) * jnp.arange(half, dtype=jnp.float32))
    angle = places.astype(jnp.float32)[..., None, None] * freq
    cosine = jnp.cos(angle)
    sine = jnp.sin(angle)
    first = vectors[..., :half]
    second = vectors[..., half:]
    return jnp.concatenate([first * cosine - second * sine, second * cosine + first * sine], -1)


def rotate_round(summed, places, kv_heads):
    number = summed.shape[0]
    turned = rotary(summed[:, : kv_heads * HD].reshape(number, kv_heads, HD), places)
    turned = turned.astype(jnp.bfloat16).reshape(number, kv_heads * HD)
    return jnp.concatenate([turned, summed[:, kv_heads * HD :].astype(jnp.bfloat16)], 1)


def own_pair(packed, head_group, kv_heads):
    key_part = lax.dynamic_slice_in_dim(packed, head_group * HD, HD, 1)
    value_part = lax.dynamic_slice_in_dim(packed, (kv_heads + head_group) * HD, HD, 1)
    return jnp.concatenate([key_part, value_part], 1)


def general(
    prompt_owner,
    fork_map,
    page_table,
    prompt_length,
    span_states,
    decode_states,
    decode_queries,
    key_weight,
    value_weight,
    out_weight,
    page_pool,
):
    replica = lax.axis_index("replica")
    device_rank = lax.axis_index("tensor")
    n_replica = lax.axis_size("replica")
    n_tensor = lax.axis_size("tensor")
    span = span_states.shape[0]
    rows, steps, width = decode_states.shape
    heads_dev = decode_queries.shape[2] // HD
    kv_heads = key_weight.shape[1] // HD
    sharing = n_tensor // kv_heads
    prompts = jnp.arange(n_replica, dtype=jnp.int32)
    own_prompt = jnp.sum(jnp.where(prompts == replica, prompt_owner, 0))
    own_length = jnp.sum(jnp.where(prompts == own_prompt, prompt_length, 0))
    row_hits = fork_map[:, None] == prompts[None, :]
    row_length = jnp.sum(jnp.where(row_hits, prompt_length[None, :], 0), 1)
    positions = jnp.concatenate(
        [
            own_length + jnp.arange(span, dtype=jnp.int32),
            (row_length[:, None] + span + jnp.arange(steps, dtype=jnp.int32)[None, :]).reshape(-1),
        ]
    )
    tokens = jnp.concatenate([span_states, decode_states.reshape(rows * steps, width)], 0)
    projected = jnp.dot(
        tokens, jnp.concatenate([key_weight, value_weight], 1), preferred_element_type=jnp.float32
    )
    share = lax.psum_scatter(projected, "tensor", scatter_dimension=0, tiled=True)
    number = share.shape[0]
    start = device_rank * number
    places = lax.dynamic_slice_in_dim(positions, start, number)
    turned = rotate_round(share, places, kv_heads)
    groups = jnp.stack(
        [own_pair(turned, group_index, kv_heads) for group_index in range(kv_heads)], 0
    )
    outgoing = jnp.repeat(groups, sharing, axis=0)
    paired = lax.all_to_all(outgoing, "tensor", split_axis=0, concat_axis=1, tiled=True).reshape(
        -1, 2 * HD
    )
    arrived = lax.all_gather(paired[:span], "replica", axis=0, tiled=True)
    tail_pair = paired[span:].reshape(rows, steps, 2 * HD)
    pool_pages = page_table.shape[0]
    cpages = pool_pages // n_replica
    page_size = page_pool.shape[2]
    entries = jnp.arange(pool_pages, dtype=jnp.int32)
    page_hits = page_table[None, :] == entries[:, None]
    page_prompt = jnp.sum(jnp.where(page_hits, entries[None, :] // cpages, 0), 1)
    page_slot = jnp.sum(jnp.where(page_hits, entries[None, :] % cpages, 0), 1)
    page_length = jnp.sum(
        jnp.where(page_prompt[:, None] == prompts[None, :], prompt_length[None, :], 0), 1
    )
    visible = (
        page_slot[:, None] * page_size + jnp.arange(page_size, dtype=jnp.int32)[None, :]
        < page_length[:, None]
    )
    pool_prompt = jnp.where(visible, page_prompt[:, None], -1).reshape(-1)
    key_prompt = jnp.concatenate([pool_prompt, jnp.repeat(prompt_owner, span)])
    key_table = jnp.concatenate([page_pool.reshape(-1, 2 * HD), arrived], 0)
    cached_keys = key_table[:, :HD]
    cached_values = key_table[:, HD:]
    scale = 1.0 / math.sqrt(HD)
    causal = jnp.arange(steps)[None, :] <= jnp.arange(steps)[:, None]
    per_block = max(1, min(rows, 512 // (steps * heads_dev)))
    blocks = rows // per_block
    queries = decode_queries.reshape(blocks, per_block, steps, heads_dev, HD)

    def attend(items):
        query, prompt, own_tail = items
        flat = query.reshape(-1, HD)
        scores = (
            lax.dot_general(
                flat, cached_keys, (((1,), (1,)), ((), ())), preferred_element_type=jnp.float32
            )
            * scale
        )
        scores = scores.reshape(per_block, steps, heads_dev, -1)
        allowed = (key_prompt[None, :] == prompt[:, None])[:, None, None, :]
        scores = jnp.where(allowed, scores, -jnp.inf)
        tail_scores = (
            jnp.einsum(
                "rshd,rtd->rsht", query, own_tail[..., :HD], preferred_element_type=jnp.float32
            )
            * scale
        )
        tail_scores = jnp.where(causal[None, :, None, :], tail_scores, -jnp.inf)
        highest = jnp.maximum(jnp.max(scores, -1), jnp.max(tail_scores, -1))
        weight = jnp.exp(scores - highest[..., None])
        tail_weight = jnp.exp(tail_scores - highest[..., None])
        total = jnp.sum(weight, -1) + jnp.sum(tail_weight, -1)
        rounded = weight.astype(jnp.bfloat16).reshape(-1, weight.shape[-1])
        mixed = jnp.dot(rounded, cached_values, preferred_element_type=jnp.float32).reshape(
            per_block, steps, heads_dev, HD
        )
        mixed = mixed + jnp.einsum(
            "rsht,rtd->rshd",
            tail_weight.astype(jnp.bfloat16),
            own_tail[..., HD:],
            preferred_element_type=jnp.float32,
        )
        return (mixed / total[..., None]).astype(jnp.bfloat16)

    attended = lax.map(
        attend,
        (
            queries,
            fork_map.reshape(blocks, per_block),
            tail_pair.reshape(blocks, per_block, steps, 2 * HD),
        ),
    )
    head_rows = attended.reshape(rows * steps, heads_dev * HD)
    decoded = jnp.dot(
        lax.all_gather(head_rows, "tensor", axis=1, tiled=True),
        out_weight,
        preferred_element_type=jnp.float32,
    )
    return decoded.astype(jnp.bfloat16).reshape(rows, steps, width)


MESH_ID = pl.DeviceIdType.MESH
TILE = 128
FAR = -(2.0**100)


def nt(left, right):
    return lax.dot_general(
        left, right, (((1,), (1,)), ((), ())), preferred_element_type=jnp.float32
    )


def fused(
    n, n_rep, steps, owner_of, forks, table, length, freq, first_tok, wk, wv,
    decode_hbm, query_hbm, pool_hbm, w_hbm, out,
    w_all, later_tok, query, pool, tok, cosine, sine, hot, mine, part, landed, span_all,
    keys, values, tail_key, tail_value, asked_all, gathered, acc,
    in_sem, rs_send, rs_recv, sp_send, sp_recv, ag_send, ag_recv,
):
    z = lax.axis_index("tensor")
    rep = lax.axis_index("replica")
    span = span_all.shape[1]
    rows = query.shape[0]
    number = rows * steps
    width = query.shape[2]
    heads = width // HD
    pages, page_size = pool.shape[0], pool.shape[1]
    cpages = pages // n_rep
    cached = pages * page_size
    span_blocks = span // TILE
    chunks = number // TILE
    blocks = span_blocks + chunks
    sampled = TILE // steps

    loads = [
        pltpu.make_async_copy(source, target, in_sem.at[index])
        for index, (source, target) in enumerate(
            ((decode_hbm, later_tok), (query_hbm, query), (pool_hbm, pool), (w_hbm, w_all))
        )
    ]
    for load in loads:
        load.start()
    barrier = pltpu.get_barrier_semaphore()
    for k in range(1, n):
        pl.semaphore_signal(
            barrier, inc=1, device_id={"tensor": lax.rem(z + k, n)}, device_id_type=MESH_ID
        )
    for k in range(1, n_rep):
        pl.semaphore_signal(
            barrier, inc=1, device_id={"replica": lax.rem(rep + k, n_rep)}, device_id_type=MESH_ID
        )
    pl.semaphore_wait(barrier, n + n_rep - 2)

    def at(block):
        return pl.ds(pl.multiple_of(block * TILE, TILE), TILE)

    def rs_copy(side, owner, block):
        return pltpu.make_async_remote_copy(
            src_ref=part.at[owner, at(block)],
            dst_ref=landed.at[side, owner, at(block)],
            send_sem=rs_send.at[owner, block],
            recv_sem=rs_recv.at[side, owner, block],
            device_id={"tensor": z + 1 if side == 0 else z - 1},
            device_id_type=MESH_ID,
        )

    tok[:span, :] = first_tok[...]
    loads[0].wait()

    @pl.loop(0, chunks)
    def _(chunk):
        tok[at(chunk + span_blocks), :] = later_tok[pl.ds(chunk * sampled, sampled)].reshape(
            TILE, tok.shape[1]
        )

    @pl.loop(0, n)
    def _(index):
        owner = lax.rem(z + n - 1 - index, n)
        column = pl.ds(pl.multiple_of(owner * HD, HD), HD)
        weight = jnp.concatenate([wk[:, column], wv[:, column]], 1)
        mine[owner] = jnp.dot(tok[...], weight, preferred_element_type=jnp.float32)
        for side, edge in ((0, z == 0), (1, z == n - 1)):

            @pl.when(edge & (index < n - 1))
            def _():
                part[owner] = mine[owner].astype(jnp.bfloat16)
                for block in range(blocks):
                    rs_copy(side, owner, block).start()

    def onward(side, block):
        for k in range(n - 1, 0, -1):
            owner = z + k if side == 0 else z - k
            inner = (z > 0) & (owner < n) if side == 0 else (z < n - 1) & (owner >= 0)

            @pl.when(inner)
            def _():
                rs_copy(side, owner, block).wait_recv()
                total = mine[owner, at(block), :] + landed[side, owner, at(block), :].astype(
                    jnp.float32
                )
                part[owner, at(block), :] = total.astype(jnp.bfloat16)
                rs_copy(side, owner, block).start()

    def forward(block):
        @pl.when(z < n // 2)
        def _():
            onward(0, block)
            onward(1, block)

        @pl.when(z >= n // 2)
        def _():
            onward(1, block)
            onward(0, block)

    line = lax.broadcasted_iota(jnp.int32, (TILE, TILE), 0)
    lane = lax.broadcasted_iota(jnp.int32, (TILE, TILE), 1)
    turn = jnp.where(lane < HD // 2, -1.0, 1.0)

    def angles(block, places):
        angle = places.astype(jnp.float32) * freq[:1, :]
        cosine[at(block), :] = jnp.cos(angle)
        sine[at(block), :] = jnp.sin(angle) * turn

    own_length = length[owner_of[rep]]
    for block in range(span_blocks):
        angles(block, own_length + block * TILE + line)

    forward(0)

    group = 8 // math.gcd(8, steps)
    small = lax.broadcasted_iota(jnp.int32, (group * steps, HD), 0)

    @pl.loop(0, rows // group)
    def _(item):
        prompt = jnp.full((group * steps, HD), forks[item * group], jnp.int32)
        for offset in range(1, group):
            prompt = jnp.where(small >= offset * steps, forks[item * group + offset], prompt)
        hot[pl.ds(pl.multiple_of(item * group * steps, 8), group * steps), :] = prompt

    @pl.loop(0, chunks)
    def _(chunk):
        prompt = hot[at(chunk), :]
        places = span + lax.rem(line, steps)
        for p in range(n_rep):
            places = places + jnp.where(prompt == p, length[p], 0)
        angles(chunk + span_blocks, places)

    loads[2].wait()
    strip = lax.broadcasted_iota(jnp.int32, (page_size, HD), 0)
    strip_lane = lax.broadcasted_iota(jnp.int32, (page_size, HD), 1)
    for page in range(pages):
        entry = jnp.int32(0)
        for index in range(pages):
            entry = jnp.where(table[index] == page, index, entry)
        prompt = entry // cpages
        seen = strip + lax.rem(entry, cpages) * page_size < length[prompt]
        here = slice(page * page_size, (page + 1) * page_size)
        keys[here, :HD] = pool[page, :, :HD]
        values[here, :HD] = pool[page, :, HD:]
        good = (seen & (strip_lane == prompt)) | (strip_lane >= n_rep)
        keys[here, HD:] = jnp.where(good, 0.0, FAR).astype(jnp.bfloat16)
    for p in range(n_rep):
        block_lane = lax.broadcasted_iota(jnp.int32, (span, HD), 1)
        good = (block_lane == owner_of[p]) | (block_lane >= n_rep)
        keys[cached + p * span : cached + (p + 1) * span, HD:] = jnp.where(good, 0.0, FAR).astype(
            jnp.bfloat16
        )
    values[:, HD:] = jnp.ones((values.shape[0], HD), jnp.bfloat16)
    tail_value[:, HD:] = jnp.ones((TILE, HD), jnp.bfloat16)

    for block in range(1, span_blocks + 1):
        forward(block)

    def reduced(block):
        for side, inside in ((0, z > 0), (1, z < n - 1)):

            @pl.when(inside)
            def _():
                rs_copy(side, z, block).wait_recv()
                mine[z, at(block), :] += landed[side, z, at(block), :].astype(jnp.float32)

        total = mine[z, at(block), :]
        key = total[:, :HD]
        key = key * cosine[at(block), :] + pltpu.roll(key, HD // 2, 1) * sine[at(block), :]
        return key.astype(jnp.bfloat16), total[:, HD:].astype(jnp.bfloat16)

    @pl.loop(0, span_blocks)
    def _(block):
        key, value = reduced(block)
        span_all[rep, at(block), :HD] = key
        span_all[rep, at(block), HD:] = value

    def sp_copy(k, whose):
        return pltpu.make_async_remote_copy(
            src_ref=span_all.at[whose],
            dst_ref=span_all.at[whose],
            send_sem=sp_send.at[k - 1],
            recv_sem=sp_recv.at[k - 1],
            device_id={"replica": lax.rem(rep + k, n_rep)},
            device_id_type=MESH_ID,
        )

    for k in range(1, n_rep):
        sp_copy(k, rep).start()
    loads[1].wait()
    for k in range(1, n_rep):
        sp_copy(k, lax.rem(rep - k + n_rep, n_rep)).wait_recv()
    for p in range(n_rep):
        keys[cached + p * span : cached + (p + 1) * span, :HD] = span_all[p, :, :HD]
        values[cached + p * span : cached + (p + 1) * span, :HD] = span_all[p, :, HD:]

    def ag_copy(side, distance, chunk, origin):
        target = z + 1 if side == 0 else z - 1
        return pltpu.make_async_remote_copy(
            src_ref=gathered.at[origin, at(chunk)],
            dst_ref=gathered.at[origin, at(chunk)],
            send_sem=ag_send.at[side, distance - 1, chunk],
            recv_sem=ag_recv.at[side, distance - 1, chunk],
            device_id={"tensor": target},
            device_id_type=MESH_ID,
        )

    def relay(distance, chunk):
        for side, origin, inside, further in (
            (0, z - distance, z >= distance, z + 1 < n),
            (1, z + distance, z + distance < n, z > 0),
        ):

            @pl.when(inside)
            def _():
                ag_copy(side, distance, chunk, origin).wait_recv()

            if distance < n - 1:

                @pl.when(inside & further)
                def _():
                    ag_copy(side, distance + 1, chunk, origin).start()

    factor = math.log2(math.e) / math.sqrt(HD)

    @pl.loop(0, chunks)
    def _(chunk):
        key, value = reduced(chunk + span_blocks)
        tail_key[...] = key
        tail_value[:, :HD] = value
        asked_all[...] = query[pl.ds(chunk * sampled, sampled)].reshape(TILE, width)
        choice = (hot[at(chunk), :] == lane).astype(jnp.bfloat16)
        causal = (line // steps == lane // steps) & (lane <= line)

        @pl.loop(0, heads, unroll=2 if heads % 2 == 0 else 1)
        def _(head):
            column = pl.ds(pl.multiple_of(head * HD, HD), HD)
            asked = asked_all[:, column]
            scores = nt(jnp.concatenate([asked, choice], 1), keys[...])
            tail = jnp.where(causal, nt(asked, tail_key[...]), FAR)
            highest = jnp.maximum(
                jnp.max(scores, 1, keepdims=True), jnp.max(tail, 1, keepdims=True)
            )
            weight = jnp.exp2((scores - highest) * factor).astype(jnp.bfloat16)
            tail_weight = jnp.exp2((tail - highest) * factor).astype(jnp.bfloat16)
            mixed = jnp.dot(weight, values[...], preferred_element_type=jnp.float32) + jnp.dot(
                tail_weight, tail_value[...], preferred_element_type=jnp.float32
            )
            gathered[z, at(chunk), column] = (mixed[:, :HD] / mixed[:, HD:]).astype(jnp.bfloat16)

        @pl.when(z + 1 < n)
        def _():
            ag_copy(0, 1, chunk, z).start()

        @pl.when(z > 0)
        def _():
            ag_copy(1, 1, chunk, z).start()

        @pl.when(chunk + span_blocks + 1 < blocks)
        def _():
            forward(chunk + span_blocks + 1)

        @pl.when(chunk > 0)
        def _():
            relay(1, chunk - 1)

    relay(1, chunks - 1)
    loads[3].wait()
    tall = min(2 * TILE, number)
    per = tall // TILE
    wide = min(512, acc.shape[1])

    def add(origin, half, first):
        span_rows = pl.ds(pl.multiple_of(half * tall, tall), tall)
        deep = pl.ds(pl.multiple_of(origin * width, width), width)

        @pl.loop(0, acc.shape[1] // wide)
        def _(column):
            cols = pl.ds(pl.multiple_of(column * wide, wide), wide)
            term = jnp.dot(
                gathered[origin, span_rows, :], w_all[deep, cols], preferred_element_type=jnp.float32
            )
            if first:
                acc[span_rows, cols] = term
            else:
                acc[span_rows, cols] += term

    @pl.loop(0, number // tall)
    def _(half):
        add(z, half, True)

    for distance in range(1, n):

        @pl.loop(0, number // tall)
        def _(half):
            if distance > 1:
                for piece in range(per):
                    relay(distance, half * per + piece)

            for side, origin, inside in (
                (0, z - distance, z >= distance),
                (1, z + distance, z + distance < n),
            ):

                @pl.when(inside)
                def _():
                    add(origin, half, False)

    @pl.loop(0, chunks)
    def _(chunk):
        out[pl.ds(chunk * sampled, sampled)] = (
            acc[at(chunk), :].astype(jnp.bfloat16).reshape(sampled, steps, acc.shape[1])
        )

    for k in range(1, n):
        for side, owner, inside in ((0, z + k, z + k < n), (1, z - k, z - k >= 0)):

            @pl.when(inside)
            def _():
                @pl.loop(0, blocks)
                def _(block):
                    rs_copy(side, owner, block).wait_send()

    for k in range(1, n_rep):
        sp_copy(k, rep).wait_send()
    for distance in range(1, n):

        @pl.loop(0, chunks)
        def _(chunk):
            @pl.when((z >= distance - 1) & (z + 1 < n))
            def _():
                ag_copy(0, distance, chunk, z - distance + 1).wait_send()

            @pl.when((z + distance - 1 < n) & (z > 0))
            def _():
                ag_copy(1, distance, chunk, z + distance - 1).wait_send()


def on_device(
    prompt_owner,
    fork_map,
    page_table,
    prompt_length,
    span_states,
    decode_states,
    decode_queries,
    key_weight,
    value_weight,
    out_weight,
    page_pool,
):
    n_replica = lax.axis_size("replica")
    n_tensor = lax.axis_size("tensor")
    span = span_states.shape[0]
    rows, steps, width = decode_states.shape
    heads_dev = decode_queries.shape[2] // HD
    kv_heads = key_weight.shape[1] // HD
    number = rows * steps
    if (
        kv_heads != n_tensor
        or span % TILE
        or number % TILE
        or number % min(2 * TILE, number)
        or TILE % steps
        or 8 % steps
        or rows % 8
        or n_replica > HD
    ):
        return general(
            prompt_owner, fork_map, page_table, prompt_length, span_states, decode_states,
            decode_queries, key_weight, value_weight, out_weight, page_pool,
        )
    half = HD // 2
    freq = np.float64(rope_base) ** (-(2.0 / HD) * np.arange(half))
    freq = jnp.asarray(np.tile(freq, (8, 2)), jnp.float32)
    pages, page_size = page_pool.shape[1:3]
    features = out_weight.shape[1]
    table = pages * page_size + n_replica * span
    total = span + number
    vmem = pl.BlockSpec(memory_space=pltpu.VMEM)
    smem = pl.BlockSpec(memory_space=pltpu.SMEM)
    hbm = pl.BlockSpec(memory_space=pl.ANY)
    bf16, f32 = jnp.bfloat16, jnp.float32
    return pl.pallas_call(
        functools.partial(fused, n_tensor, n_replica, steps),
        name="fused",
        out_shape=jax.ShapeDtypeStruct((rows, steps, features), bf16),
        in_specs=[smem] * 4 + [vmem] * 4 + [hbm] * 4,
        out_specs=vmem,
        scratch_shapes=[
            pltpu.VMEM(out_weight.shape, bf16),
            pltpu.VMEM(decode_states.shape, bf16),
            pltpu.VMEM(decode_queries.shape, bf16),
            pltpu.VMEM(page_pool.shape[1:], bf16),
            pltpu.VMEM((total, width), bf16),
            pltpu.VMEM((total, HD), f32),
            pltpu.VMEM((total, HD), f32),
            pltpu.VMEM((number, HD), jnp.int32),
            pltpu.VMEM((n_tensor, total, 2 * HD), f32),
            pltpu.VMEM((n_tensor, total, 2 * HD), bf16),
            pltpu.VMEM((2, n_tensor, total, 2 * HD), bf16),
            pltpu.VMEM((n_replica, span, 2 * HD), bf16),
            pltpu.VMEM((table, 2 * HD), bf16),
            pltpu.VMEM((table, 2 * HD), bf16),
            pltpu.VMEM((TILE, HD), bf16),
            pltpu.VMEM((TILE, 2 * HD), bf16),
            pltpu.VMEM((TILE, heads_dev * HD), bf16),
            pltpu.VMEM((n_tensor, number, heads_dev * HD), bf16),
            pltpu.VMEM((number, features), f32),
            pltpu.SemaphoreType.DMA((4,)),
            pltpu.SemaphoreType.DMA((n_tensor, total // TILE)),
            pltpu.SemaphoreType.DMA((2, n_tensor, total // TILE)),
            pltpu.SemaphoreType.DMA((n_replica - 1,)),
            pltpu.SemaphoreType.DMA((n_replica - 1,)),
            pltpu.SemaphoreType.DMA((2, n_tensor - 1, number // TILE)),
            pltpu.SemaphoreType.DMA((2, n_tensor - 1, number // TILE)),
        ],
        compiler_params=pltpu.CompilerParams(
            collective_id=0, has_side_effects=True, vmem_limit_bytes=63 * 1024 * 1024
        ),
    )(
        prompt_owner, fork_map, page_table, prompt_length, freq, span_states, key_weight,
        value_weight, decode_states, decode_queries, page_pool[0], out_weight,
    )


def solution(mesh):
    in_specs = (
        P("parts"),
        P(("parts", "replica")),
        P("parts"),
        P("parts"),
        P(("parts", "replica"), "tensor"),
        P(("parts", "replica"), None, "tensor"),
        P(("parts", "replica"), None, "tensor"),
        P("tensor", None),
        P("tensor", None),
        P(None, "tensor"),
        P("tensor", "parts", None, None),
    )
    out_specs = P(("parts", "replica"), None, "tensor")
    return jax.shard_map(
        on_device, mesh=mesh, in_specs=in_specs, out_specs=out_specs, check_vma=False
    )
```
